32 devices in a mesh: rep: 4 (over x, y), dp: 8 (over z, core).
Axes of the slice: x: 2, y: 2, z: 4, core: 2. Of those that a mesh axis runs over, the one named last changes fastest.
Arguments:
- x: bfloat16 [32, 4096, 640], P(('rep', 'dp')), parts along dimension 0
- dy: bfloat16 [32, 4096, 640], P(('rep', 'dp')), parts along dimension 0
- w_gate: bfloat16 [2, 640, 3200], P(None, 'dp')
- w_up: bfloat16 [2, 640, 3200], P(None, 'dp')
- w_down: bfloat16 [2, 3200, 640], P(None, 'dp')
Outputs:
- output 1: bfloat16 [32, 4096, 640], P(('rep', 'dp')), parts along dimension 0
- output 2: bfloat16 [8, 640, 3200], P('rep', 'dp'), parts along dimension 0
- output 3: bfloat16 [8, 640, 3200], P('rep', 'dp'), parts along dimension 0
- output 4: bfloat16 [8, 3200, 640], P('rep', 'dp'), parts along dimension 0
There are 4 independent parts. The reference program is written for one: setup_inputs(seed, part) draws one part's arguments, and reference() takes and returns one part's arrays. A program takes and returns all parts, laid end to end along the dimension named above; an argument that names none is the same for every part.
All inputs are finite; a program needn't handle non-finite values.
Results may differ from the reference program's by a relative error of at most 0.018.
Values are sent between devices in bfloat16 or wider.
A program may use at most 2 GiB of HBM per device.

```python
import jax
import jax.numpy as jnp
from jax import lax

SEQUENCES = 8
TOKENS = 4096
D = 640
FF = 3200
LAYERS = 2
NAMES = ("w_gate", "w_up", "w_down")
SHAPES = {"w_gate": (LAYERS, D, FF), "w_up": (LAYERS, D, FF), "w_down": (LAYERS, FF, D)}


def bump(key, n, height):
    away = (jnp.arange(n, dtype=jnp.int32) - jax.random.randint(key, (), 0, n, jnp.int32)) % n
    return jnp.where(away < n // 8, height, 1.0)


def together(key, own, strength):
    shared = jax.random.normal(key, own.shape[1:], jnp.float32)
    return (own + strength * shared) * lax.rsqrt(1 + strength * strength)


def setup_inputs(seed: int = 0, part: int = 0) -> dict:
    kx, kdy, ka, kb, kz, kf, kh, kl, *kw = jax.random.split(jax.random.key(seed), 8 + len(NAMES))
    kx, kdy, ka, kb = (jax.random.fold_in(k, part) for k in (kx, kdy, ka, kb))
    shape = (SEQUENCES, TOKENS, D)
    much_x, much_dy = jax.random.uniform(kz, (2,), jnp.float32, 0.0, 1.0)
    layers = 2.0 ** jax.random.uniform(kl, (LAYERS, 1, 1), jnp.float32, -1.0, 1.0)
    x = together(ka, jax.random.normal(kx, shape, jnp.float32), much_x) * bump(kf, D, 4.0)
    dy = together(kb, jax.random.normal(kdy, shape, jnp.float32), much_dy)
    drawn = {"x": x.astype(jnp.bfloat16), "dy": (dy * (SEQUENCES * TOKENS) ** -0.5).astype(jnp.bfloat16)}
    for key, name in zip(kw, NAMES, strict=True):
        w = jax.random.normal(key, SHAPES[name], jnp.float32) * SHAPES[name][1] ** -0.5
        drawn[name] = (w * {"w_gate": 1.0, "w_up": bump(kh, FF, 4.0), "w_down": layers}[name]).astype(jnp.bfloat16)
    return drawn


def matmul(a, w):
    return jnp.dot(a, w, preferred_element_type=jnp.float32).astype(jnp.bfloat16)


def normed(h):
    wide = h.astype(jnp.float32)
    scale = lax.rsqrt(jnp.mean(wide**2, -1, keepdims=True) + 1e-6)
    return (wide * scale).astype(jnp.bfloat16)


def layer(h, w):
    a = normed(h)
    gate = jnp.dot(a, w["w_gate"], preferred_element_type=jnp.float32)
    up = jnp.dot(a, w["w_up"], preferred_element_type=jnp.float32)
    return h + matmul((jax.nn.silu(gate) * up).astype(jnp.bfloat16), w["w_down"])


def stack(weights, h):
    return lax.scan(lambda h, w: (layer(h, w), None), h, weights)[0]


def reference(x, dy, w_gate, w_up, w_down):
    weights = dict(zip(NAMES, (w_gate, w_up, w_down), strict=True))

    def take(so_far, sequence):
        h, by_y = sequence
        _, back = jax.vjp(stack, weights, h)
        by_weights, by_h = back(by_y)
        return jax.tree.map(lambda total, term: total + term.astype(jnp.float32), so_far, by_weights), by_h

    none_yet = {name: jnp.zeros(w.shape, jnp.float32) for name, w in weights.items()}
    by_weights, by_x = lax.scan(take, none_yet, (x, dy))
    return (by_x, *(by_weights[name].astype(jnp.bfloat16) for name in NAMES))
```

```python
import functools

import jax
import jax.numpy as jnp
from jax import lax
from jax.experimental import pallas as pl
from jax.experimental.pallas import tpu as pltpu
from jax.sharding import PartitionSpec as P

TOKENS, D, FF = 4096, 640, 3200
BLOCK = 640
BLOCKS = FF // BLOCK
VMEM = 62 * 1024 * 1024
F32, BF16 = jnp.float32, jnp.bfloat16


def nn(a, b):
    return lax.dot_general(a, b, (((1,), (0,)), ((), ())), preferred_element_type=F32)


def nt(a, b):
    return lax.dot_general(a, b, (((1,), (1,)), ((), ())), preferred_element_type=F32)


def tn(a, b):
    return lax.dot_general(a, b, (((0,), (0,)), ((), ())), preferred_element_type=F32)


def params(*semantics):
    return pltpu.CompilerParams(dimension_semantics=semantics, vmem_limit_bytes=VMEM)


def cost(flops, nbytes):
    return pl.CostEstimate(flops=flops, bytes_accessed=nbytes, transcendentals=0)


MM = 2 * TOKENS * D * FF


def scale_of(wide):
    return lax.rsqrt(jnp.mean(wide * wide, -1, keepdims=True) + 1e-6)


ZS, CORES = 4, 2
GU_ROWS, D_ROWS = D // 8, FF // 8


def pieces_of():
    out = []
    for buffer in range(4):
        for n in range(10 if buffer % 2 == 0 else 5):
            width = 640 if buffer % 2 == 0 else 128
            out.append((buffer, pl.ds(n * width, width), n % 2))
    return out


PIECES = pieces_of()


def gate_up_kernel(sub, a_ref, gu0, d0, gu1, d1, gu_ref, p_ref, o0, o1, o2, o3, b0, b1, b2, b3, own_sem, out_sem, send_z, send_x, send_d, arrive, crossed):
    r, dp = lax.axis_index("rep"), lax.axis_index("dp")
    z, k = dp // 2, dp % 2
    relay = r % 2 == k
    side = r // 2
    buffers, outs, shards = (b0, b1, b2, b3), (o0, o1, o2, o3), (gu0, d0, gu1, d1)
    step = pl.program_id(0) * pl.num_programs(1) + pl.program_id(1)
    steps = BLOCKS * (TOKENS // a_ref.shape[0])
    count = len(PIECES)

    def send(q, at, to, sem, to_sem):
        ref = buffers[PIECES[q][0]].at[at, k, :, PIECES[q][1]]
        return pltpu.make_async_remote_copy(
            src_ref=ref, dst_ref=ref, send_sem=sem, recv_sem=to_sem, device_id=to, device_id_type=pl.DeviceIdType.MESH
        )

    def three(q, sem):
        ref = buffers[PIECES[q][0]].at[pl.ds(0, 3), 0, :, PIECES[q][1]]
        return pltpu.make_async_copy(ref, ref, sem)

    def relays(q):
        return jnp.logical_and(relay, side == PIECES[q][2])

    def along(q):
        @pl.when(relays(q))
        def _():
            for dz in (1, 2, 3):
                to = (r, lax.rem(z + dz, ZS) * 2 + k)
                send(q, z, to, send_z.at[q], arrive.at[q]).start()

    def across(q):
        @pl.when(relays(q))
        def _():
            three(q, arrive.at[q]).wait()
            for dr in (1, 2, 3):
                for dz in (1, 2, 3):
                    to = (lax.rem(r + dr, 4), dp)
                    send(q, lax.rem(z + dz, ZS), to, send_x.at[q, dr - 1], arrive.at[q]).start()

    def cross(q):
        ref = buffers[PIECES[q][0]].at[:, k, :, PIECES[q][1]]
        return pltpu.make_async_remote_copy(
            src_ref=ref,
            dst_ref=ref,
            send_sem=send_d.at[q],
            recv_sem=crossed.at[q],
            device_id=(r, z * 2 + 1 - k),
            device_id_type=pl.DeviceIdType.MESH,
        )

    def over(q):
        @pl.when(jnp.logical_not(relays(q)))
        def _():
            three(q, arrive.at[q]).wait()

        cross(q).start()

    def arrived(q):
        cross(q).wait_recv()

    def end(q):
        cross(q).wait_send()

        @pl.when(relays(q))
        def _():
            three(q, send_z.at[q]).wait()
            for dr in range(3):
                three(q, send_x.at[q, dr]).wait()

    def to_hbm(n):
        return pltpu.make_async_copy(buffers[n], outs[n], out_sem.at[n])

    @pl.when(step == 0)
    def _():
        own = [pltpu.make_async_copy(shards[n], buffers[n].at[z, k], own_sem.at[n]) for n in range(4)]
        for copy in own:
            copy.start()
        barrier = pltpu.get_barrier_semaphore()
        for n in (1, 2, 3):
            pl.semaphore_signal(
                barrier, inc=1, device_id=(r, lax.rem(z + n, ZS) * 2 + k), device_id_type=pl.DeviceIdType.MESH
            )
            pl.semaphore_signal(barrier, inc=1, device_id=(lax.rem(r + n, 4), dp), device_id_type=pl.DeviceIdType.MESH)
        pl.semaphore_signal(barrier, inc=1, device_id=(r, z * 2 + 1 - k), device_id_type=pl.DeviceIdType.MESH)
        pl.semaphore_wait(barrier, 7)
        for copy in own:
            copy.wait()
        for q in range(count):
            along(q)
        across(0)
        across(1)
        over(0)
        over(1)
        across(2)
        arrived(0)
        arrived(1)

    @pl.when(step == 1)
    def _():
        across(3)
        across(4)
        over(2)

    for s in range(2, steps):

        @pl.when(step == s)
        def _():
            across(s + 3)
            over(s + 1)
            arrived(s)

    cols = pl.ds(pl.multiple_of(pl.program_id(0) * (2 * BLOCK), 2 * BLOCK), 2 * BLOCK)
    w = b0[:, :, :, cols].reshape(D, 2 * BLOCK)
    for s in range(a_ref.shape[0] // sub):
        rows = pl.ds(s * sub, sub)
        gu = nn(a_ref[rows, :], w)
        gu_ref[rows, :] = gu
        gate, up = gu[:, :BLOCK], gu[:, BLOCK:]
        p_ref[rows, :] = (gate * jax.nn.sigmoid(gate) * up).astype(BF16)

    @pl.when(step == steps - 1)
    def _():
        for q in range(steps + 3, count):
            across(q)
            over(q - 2)
        over(count - 2)
        over(count - 1)
        for q in range(steps, count):
            arrived(q)
        for n in range(4):
            to_hbm(n).start()
        for q in range(count):
            end(q)
        for n in range(4):
            to_hbm(n).wait()


def gate_up(a, gu0, d0, gu1, d1, tile=1024, sub=1024):
    hbm = pl.BlockSpec(memory_space=pl.ANY)
    wide = (ZS, CORES, GU_ROWS, 2 * FF)
    tall = (ZS, CORES, D_ROWS, D)
    count = len(PIECES)
    dma = pltpu.SemaphoreType.DMA
    return pl.pallas_call(
        functools.partial(gate_up_kernel, sub),
        grid=(BLOCKS, TOKENS // tile),
        in_specs=[pl.BlockSpec((tile, D), lambda j, i: (i, 0)), hbm, hbm, hbm, hbm],
        out_specs=[
            pl.BlockSpec((tile, 2 * BLOCK), lambda j, i: (i, j)),
            pl.BlockSpec((tile, BLOCK), lambda j, i: (i, j)),
            hbm,
            hbm,
            hbm,
            hbm,
        ],
        out_shape=[
            jax.ShapeDtypeStruct((TOKENS, 2 * FF), F32),
            jax.ShapeDtypeStruct((TOKENS, FF), BF16),
            jax.ShapeDtypeStruct(wide, BF16),
            jax.ShapeDtypeStruct(tall, BF16),
            jax.ShapeDtypeStruct(wide, BF16),
            jax.ShapeDtypeStruct(tall, BF16),
        ],
        scratch_shapes=[
            pltpu.VMEM(wide, BF16),
            pltpu.VMEM(tall, BF16),
            pltpu.VMEM(wide, BF16),
            pltpu.VMEM(tall, BF16),
            dma((4,)),
            dma((4,)),
            dma((count,)),
            dma((count, 3)),
            dma((count,)),
            dma((count,)),
            dma((count,)),
        ],
        compiler_params=pltpu.CompilerParams(
            dimension_semantics=("arbitrary", "arbitrary"), vmem_limit_bytes=VMEM, collective_id=0, has_side_effects=True
        ),
        cost_estimate=cost(2 * MM, TOKENS * FF * 10),
        name="gate_up",
    )(a, gu0, d0, gu1, d1)


def down_kernel(p_ref, w_ref, h_ref, out_ref, a_ref):
    y = nn(p_ref[...], w_ref[...]).astype(BF16)
    h = h_ref[...] + y
    out_ref[...] = h
    wide = h.astype(F32)
    a_ref[...] = (wide * scale_of(wide)).astype(BF16)


def down(p, w, h, tile=512):
    row = pl.BlockSpec((tile, D), lambda i: (i, 0))
    return pl.pallas_call(
        down_kernel,
        grid=(TOKENS // tile,),
        in_specs=[
            pl.BlockSpec((tile, FF), lambda i: (i, 0)),
            pl.BlockSpec((FF, D), lambda i: (0, 0), pipeline_mode=pl.Buffered(1)),
            row,
        ],
        out_specs=[row, row],
        out_shape=[jax.ShapeDtypeStruct((TOKENS, D), BF16)] * 2,
        compiler_params=params("arbitrary"),
        cost_estimate=cost(MM, TOKENS * FF * 2),
        name="down",
    )(p, w, h)


def back_kernel(sub, again, dy_ref, wd_ref, a_ref, gu_ref, dgu_ref, dw_ref, dd_ref, acc, accd, p_ref):
    i = pl.program_id(1)

    @pl.when(i == 0)
    def _():
        acc[...] = jnp.zeros_like(acc)
        accd[...] = jnp.zeros_like(accd)

    for s in range(dy_ref.shape[0] // sub):
        rows = pl.ds(s * sub, sub)
        dp = nt(dy_ref[rows, :], wd_ref[...]).astype(BF16).astype(F32)
        if again:
            gu = nn(a_ref[rows, :], gu_ref[...])
            gate, up = gu[:, :BLOCK], gu[:, BLOCK:]
        else:
            gate, up = gu_ref[rows, :BLOCK], gu_ref[rows, BLOCK:]
        sig = jax.nn.sigmoid(gate)
        silu = gate * sig
        p_ref[rows, :] = (silu * up).astype(BF16)
        dgu_ref[rows, :BLOCK] = (dp * up * (sig * (1.0 + gate * (1.0 - sig)))).astype(BF16)
        dgu_ref[rows, BLOCK:] = (dp * silu).astype(BF16)
    acc[...] += tn(a_ref[...], dgu_ref[...])
    accd[...] += tn(p_ref[...], dy_ref[...])

    @pl.when(i == pl.num_programs(1) - 1)
    def _():
        dw_ref[...] = acc[...].astype(BF16)
        dd_ref[...] = accd[...].astype(BF16)


def back(dy, wd, a, gu, again, first, blocks, tile=1024, sub=512):
    return pl.pallas_call(
        functools.partial(back_kernel, sub, again),
        grid=(blocks, TOKENS // tile),
        in_specs=[
            pl.BlockSpec((tile, D), lambda j, i: (i, 0)),
            pl.BlockSpec((BLOCK, D), lambda j, i: (first + j, 0)),
            pl.BlockSpec((tile, D), lambda j, i: (i, 0)),
            pl.BlockSpec((D, 2 * BLOCK), lambda j, i: (0, first + j))
            if again
            else pl.BlockSpec((tile, 2 * BLOCK), lambda j, i: (i, first + j)),
        ],
        out_specs=[
            pl.BlockSpec((tile, 2 * BLOCK), lambda j, i: (i, j)),
            pl.BlockSpec((D, 2 * BLOCK), lambda j, i: (0, j)),
            pl.BlockSpec((BLOCK, D), lambda j, i: (j, 0)),
        ],
        out_shape=[
            jax.ShapeDtypeStruct((TOKENS, 2 * BLOCK * blocks), BF16),
            jax.ShapeDtypeStruct((D, 2 * BLOCK * blocks), BF16),
            jax.ShapeDtypeStruct((BLOCK * blocks, D), BF16),
        ],
        scratch_shapes=[
            pltpu.VMEM((D, 2 * BLOCK), F32),
            pltpu.VMEM((BLOCK, D), F32),
            pltpu.VMEM((tile, BLOCK), BF16),
        ],
        compiler_params=params("arbitrary", "arbitrary"),
        cost_estimate=cost((6 if again else 4) * MM * blocks // BLOCKS, TOKENS * FF * (4 if again else 12) * blocks // BLOCKS),
        name="back",
    )(dy, wd, a, gu)


def grad_in_kernel(split, one_ref, two_ref, w_ref, h_ref, dy_ref, dh_ref):
    da = nt(one_ref[...], w_ref[:, :split]) + nt(two_ref[...], w_ref[:, split:])
    da = da.astype(BF16).astype(F32)
    wide = h_ref[...].astype(F32)
    scale = scale_of(wide)
    dot = jnp.mean(da * wide, -1, keepdims=True)
    by_wide = da * scale - wide * (scale * scale * scale * dot)
    dh_ref[...] = dy_ref[...] + by_wide.astype(BF16)


def grad_in(one, two, w, h, dy, tile=512):
    row = pl.BlockSpec((tile, D), lambda i: (i, 0))
    split = one.shape[1]
    return pl.pallas_call(
        functools.partial(grad_in_kernel, split),
        grid=(TOKENS // tile,),
        in_specs=[
            pl.BlockSpec((tile, split), lambda i: (i, 0)),
            pl.BlockSpec((tile, 2 * FF - split), lambda i: (i, 0)),
            pl.BlockSpec((D, 2 * FF), lambda i: (0, 0), pipeline_mode=pl.Buffered(1)),
            row,
            row,
        ],
        out_specs=row,
        out_shape=jax.ShapeDtypeStruct((TOKENS, D), BF16),
        compiler_params=params("arbitrary"),
        cost_estimate=cost(2 * MM, TOKENS * FF * 4),
        name="grad_in",
    )(one, two, w, h, dy)


def normed(h):
    wide = h.astype(F32)
    return (wide * scale_of(wide)).astype(BF16)


def beside(gate, up):
    parts = []
    for j in range(BLOCKS):
        cols = slice(j * BLOCK, (j + 1) * BLOCK)
        parts += [gate[:, cols], up[:, cols]]
    return jnp.concatenate(parts, 1)


def apart(both):
    parts = [both[:, j * BLOCK : (j + 1) * BLOCK] for j in range(2 * BLOCKS)]
    return jnp.concatenate(parts[0::2], 1), jnp.concatenate(parts[1::2], 1)


def scatter(dw):
    return lax.psum_scatter(dw, "dp", scatter_dimension=0, tiled=True)


SPLIT = 2


def solution(mesh):
    def backward(dy, wd, a, gu, again, w, h):
        one, dw_one, dd_one = back(dy, wd, a, gu, again, 0, SPLIT)
        dy, dw_one, dd_one = lax.optimization_barrier((dy, dw_one, dd_one))
        two, dw_two, dd_two = back(dy, wd, a, gu, again, SPLIT, BLOCKS - SPLIT)
        dy, dw_two, dd_two = lax.optimization_barrier((dy, dw_two, dd_two))
        by_gu = jnp.concatenate([scatter(dw_one), scatter(dw_two)], 1)
        by_d = scatter(jnp.concatenate([dd_one, dd_two], 0))
        return grad_in(one, two, w, h, dy), apart(by_gu), by_d

    def step(x, dy, w_gate, w_up, w_down):
        h0, dy = x[0], dy[0]
        a0 = normed(h0)
        gu0, p0, w0, d0, w1, d1 = gate_up(a0, beside(w_gate[0], w_up[0]), w_down[0], beside(w_gate[1], w_up[1]), w_down[1])
        w0, w1 = w0.reshape(D, 2 * FF), w1.reshape(D, 2 * FF)
        d0, d1 = d0.reshape(FF, D), d1.reshape(FF, D)
        h1, a1 = down(p0, d0, h0)
        dh1, (g1, u1), by_d1 = backward(dy, d1, a1, w1, True, w1, h1)
        dx, (g0, u0), by_d0 = backward(dh1, d0, a0, gu0, False, w0, h0)
        return dx[None], jnp.stack([g0, g1]), jnp.stack([u0, u1]), jnp.stack([by_d0, by_d1])

    tokens = P(("rep", "dp"), None, None)
    weights = P(None, "dp", None)
    return jax.shard_map(
        step,
        mesh=mesh,
        in_specs=(tokens, tokens, weights, weights, weights),
        out_specs=(tokens,) + (P("rep", "dp", None),) * 3,
        check_vma=False,
    )
```

```python
import functools

import jax
import jax.numpy as jnp
from jax import lax
from jax.experimental import pallas as pl
from jax.experimental.pallas import tpu as pltpu
from jax.sharding import PartitionSpec as P

TOKENS, D, FF = 4096, 640, 3200
BLOCK = 640
BLOCKS = FF // BLOCK
VMEM = 62 * 1024 * 1024
F32, BF16 = jnp.float32, jnp.bfloat16


def nn(a, b):
    return lax.dot_general(a, b, (((1,), (0,)), ((), ())), preferred_element_type=F32)


def nt(a, b):
    return lax.dot_general(a, b, (((1,), (1,)), ((), ())), preferred_element_type=F32)


def tn(a, b):
    return lax.dot_general(a, b, (((0,), (0,)), ((), ())), preferred_element_type=F32)


def params(*semantics):
    return pltpu.CompilerParams(dimension_semantics=semantics, vmem_limit_bytes=VMEM)


def cost(flops, nbytes):
    return pl.CostEstimate(flops=flops, bytes_accessed=nbytes, transcendentals=0)


MM = 2 * TOKENS * D * FF


def scale_of(wide):
    return lax.rsqrt(jnp.mean(wide * wide, -1, keepdims=True) + 1e-6)


ZS, CORES = 4, 2
ROWS = D // 8


def pieces_of():
    out = []
    for buffer in range(2):
        for n in range(2 * BLOCKS):
            out.append((buffer, pl.ds(n * BLOCK, BLOCK), n % 2))
    return out


PIECES = pieces_of()


def gate_up_kernel(tile, sub, x_ref, wg, wu, gu_ref, p_ref, a_out, o0, o1, b0, b1, a_ref, own_sem, out_sem, send_z, send_x, send_d, arrive, crossed):
    r, dp = lax.axis_index("rep"), lax.axis_index("dp")
    z, k = dp // 2, dp % 2
    relay = r % 2 == k
    side = r // 2
    buffers, outs = (b0, b1), (o0, o1)
    step = pl.program_id(0) * pl.num_programs(1) + pl.program_id(1)
    steps = BLOCKS * (TOKENS // tile)
    count = len(PIECES)

    def send(q, at, to, sem, to_sem):
        ref = buffers[PIECES[q][0]].at[at, k, :, PIECES[q][1]]
        return pltpu.make_async_remote_copy(
            src_ref=ref, dst_ref=ref, send_sem=sem, recv_sem=to_sem, device_id=to, device_id_type=pl.DeviceIdType.MESH
        )

    def three(q, sem):
        ref = buffers[PIECES[q][0]].at[pl.ds(0, 3), 0, :, PIECES[q][1]]
        return pltpu.make_async_copy(ref, ref, sem)

    def relays(q):
        return jnp.logical_and(relay, side == PIECES[q][2])

    def along(q):
        @pl.when(relays(q))
        def _():
            for dz in (1, 2, 3):
                to = (r, lax.rem(z + dz, ZS) * 2 + k)
                send(q, z, to, send_z.at[q], arrive.at[q]).start()

    def across(q):
        @pl.when(relays(q))
        def _():
            three(q, arrive.at[q]).wait()
            for dr in (1, 2, 3):
                for dz in (1, 2, 3):
                    to = (lax.rem(r + dr, 4), dp)
                    send(q, lax.rem(z + dz, ZS), to, send_x.at[q, dr - 1], arrive.at[q]).start()

    def cross(q):
        ref = buffers[PIECES[q][0]].at[:, k, :, PIECES[q][1]]
        return pltpu.make_async_remote_copy(
            src_ref=ref,
            dst_ref=ref,
            send_sem=send_d.at[q],
            recv_sem=crossed.at[q],
            device_id=(r, z * 2 + 1 - k),
            device_id_type=pl.DeviceIdType.MESH,
        )

    def over(q):
        @pl.when(jnp.logical_not(relays(q)))
        def _():
            three(q, arrive.at[q]).wait()

        cross(q).start()

    def arrived(q):
        cross(q).wait_recv()

    def end(q):
        cross(q).wait_send()

        @pl.when(relays(q))
        def _():
            three(q, send_z.at[q]).wait()
            for dr in range(3):
                three(q, send_x.at[q, dr]).wait()

    def to_hbm(n):
        return pltpu.make_async_copy(buffers[n], outs[n], out_sem.at[n])

    @pl.when(step == 0)
    def _():
        for n in range(2):
            for j in range(BLOCKS):
                for m in range(2):
                    pltpu.make_async_copy(
                        (wg, wu)[m].at[n, :, pl.ds(j * BLOCK, BLOCK)],
                        buffers[n].at[z, k, :, pl.ds((2 * j + m) * BLOCK, BLOCK)],
                        own_sem.at[n],
                    ).start()
        barrier = pltpu.get_barrier_semaphore()
        for n in (1, 2, 3):
            pl.semaphore_signal(
                barrier, inc=1, device_id=(r, lax.rem(z + n, ZS) * 2 + k), device_id_type=pl.DeviceIdType.MESH
            )
            pl.semaphore_signal(barrier, inc=1, device_id=(lax.rem(r + n, 4), dp), device_id_type=pl.DeviceIdType.MESH)
        pl.semaphore_signal(barrier, inc=1, device_id=(r, z * 2 + 1 - k), device_id_type=pl.DeviceIdType.MESH)
        pl.semaphore_wait(barrier, 7)
        for n in range(2):
            ref = buffers[n].at[z, k]
            pltpu.make_async_copy(ref, ref, own_sem.at[n]).wait()
        for q in range(count):
            along(q)
        across(0)
        across(1)
        over(0)
        over(1)
        across(2)
        arrived(0)
        arrived(1)

    @pl.when(step == 1)
    def _():
        across(3)
        across(4)
        over(2)

    for s in range(2, steps):

        @pl.when(step == s)
        def _():
            if s + 3 < count:
                across(s + 3)
            if s + 1 < count:
                over(s + 1)
            if s < count:
                arrived(s)

    cols = pl.ds(pl.multiple_of(pl.program_id(0) * (2 * BLOCK), 2 * BLOCK), 2 * BLOCK)
    w = b0[:, :, :, cols].reshape(D, 2 * BLOCK)
    start = pl.program_id(1) * tile

    @pl.when(pl.program_id(0) == 0)
    def _():
        wide = x_ref[...].astype(F32)
        a_ref[pl.ds(pl.multiple_of(start, tile), tile), :] = (wide * scale_of(wide)).astype(BF16)

    @pl.when(step == TOKENS // tile)
    def _():
        pltpu.make_async_copy(a_ref, a_out, out_sem.at[2]).start()

    for s in range(tile // sub):
        rows = pl.ds(s * sub, sub)
        gu = nn(a_ref[pl.ds(pl.multiple_of(start + s * sub, sub), sub), :], w)
        gu_ref[rows, :] = gu
        gate, up = gu[:, :BLOCK], gu[:, BLOCK:]
        p_ref[rows, :] = (gate * jax.nn.sigmoid(gate) * up).astype(BF16)

    @pl.when(step == steps - 1)
    def _():
        for n in range(2):
            to_hbm(n).start()
        for q in range(count):
            end(q)
        for n in range(2):
            to_hbm(n).wait()
        pltpu.make_async_copy(a_ref, a_out, out_sem.at[2]).wait()


def gate_up(x, wg, wu, tile=1024, sub=1024):
    hbm = pl.BlockSpec(memory_space=pl.ANY)
    wide = (ZS, CORES, ROWS, 2 * FF)
    count = len(PIECES)
    last = TOKENS // tile - 1
    dma = pltpu.SemaphoreType.DMA
    return pl.pallas_call(
        functools.partial(gate_up_kernel, tile, sub),
        grid=(BLOCKS, TOKENS // tile),
        in_specs=[pl.BlockSpec((tile, D), lambda j, i: (jnp.where(j == 0, i, last), 0)), hbm, hbm],
        out_specs=[
            pl.BlockSpec((tile, 2 * BLOCK), lambda j, i: (i, j)),
            pl.BlockSpec((tile, BLOCK), lambda j, i: (i, j)),
            hbm,
            hbm,
            hbm,
        ],
        out_shape=[
            jax.ShapeDtypeStruct((TOKENS, 2 * FF), F32),
            jax.ShapeDtypeStruct((TOKENS, FF), BF16),
            jax.ShapeDtypeStruct((TOKENS, D), BF16),
            jax.ShapeDtypeStruct(wide, BF16),
            jax.ShapeDtypeStruct(wide, BF16),
        ],
        scratch_shapes=[
            pltpu.VMEM(wide, BF16),
            pltpu.VMEM(wide, BF16),
            pltpu.VMEM((TOKENS, D), BF16),
            dma((2,)),
            dma((3,)),
            dma((count,)),
            dma((count, 3)),
            dma((count,)),
            dma((count,)),
            dma((count,)),
        ],
        compiler_params=pltpu.CompilerParams(
            dimension_semantics=("arbitrary", "arbitrary"), vmem_limit_bytes=VMEM, collective_id=0, has_side_effects=True
        ),
        cost_estimate=cost(2 * MM, TOKENS * FF * 10),
        name="gate_up",
    )(x, wg, wu)


def down_kernel(p_ref, w_ref, h_ref, out_ref, a_ref, across):
    @pl.when(pl.program_id(0) == 0)
    def _():
        across[...] = w_ref[...].T

    y = nt(across[...], p_ref[...]).T.astype(BF16)
    h = h_ref[...] + y
    out_ref[...] = h
    wide = h.astype(F32)
    a_ref[...] = (wide * scale_of(wide)).astype(BF16)


def down(p, w, h, tile=1024):
    row = pl.BlockSpec((tile, D), lambda i: (i, 0))
    return pl.pallas_call(
        down_kernel,
        grid=(TOKENS // tile,),
        in_specs=[
            pl.BlockSpec((tile, FF), lambda i: (i, 0)),
            pl.BlockSpec((FF, D), lambda i: (0, 0), pipeline_mode=pl.Buffered(1)),
            row,
        ],
        out_specs=[row, row],
        out_shape=[jax.ShapeDtypeStruct((TOKENS, D), BF16)] * 2,
        scratch_shapes=[pltpu.VMEM((D, FF), BF16)],
        compiler_params=params("arbitrary"),
        cost_estimate=cost(MM, TOKENS * FF * 2),
        name="down",
    )(p, w, h)


def back_kernel(sub, again, with_d, joins, dy_ref, wd_ref, a_ref, gu_ref, *rest):
    dgu_ref, *rest = rest[1:] if joins else rest
    if with_d:
        dw_ref, dd_ref, acc, p_ref, accd = rest
    else:
        dw_ref, acc = rest
    i = pl.program_id(1)

    @pl.when(i == 0)
    def _():
        acc[...] = jnp.zeros_like(acc)
        if with_d:
            accd[...] = jnp.zeros_like(accd)

    for s in range(dy_ref.shape[0] // sub):
        rows = pl.ds(s * sub, sub)
        dp = nt(dy_ref[rows, :], wd_ref[...]).astype(BF16).astype(F32)
        if again:
            gu = nn(a_ref[rows, :], gu_ref[...])
            gate, up = gu[:, :BLOCK], gu[:, BLOCK:]
        else:
            gate, up = gu_ref[rows, :BLOCK], gu_ref[rows, BLOCK:]
        sig = jax.nn.sigmoid(gate)
        silu = gate * sig
        if with_d:
            p_ref[rows, :] = (silu * up).astype(BF16)
        dgu_ref[rows, :BLOCK] = (dp * up * (sig * (1.0 + gate * (1.0 - sig)))).astype(BF16)
        dgu_ref[rows, BLOCK:] = (dp * silu).astype(BF16)
    acc[...] += tn(a_ref[...], dgu_ref[...])
    if with_d:
        accd[...] += tn(p_ref[...], dy_ref[...])

    @pl.when(i == pl.num_programs(1) - 1)
    def _():
        dw_ref[...] = acc[...].astype(BF16)
        if with_d:
            dd_ref[...] = accd[...].astype(BF16)


def back(dy, wd, a, gu, again, with_d, first, blocks, joins=None, tile=1024, sub=512):
    spare = [jax.ShapeDtypeStruct((FF, D), BF16)] if with_d else []
    before = [] if joins is None else [joins]
    return pl.pallas_call(
        functools.partial(back_kernel, sub, again, with_d, bool(before)),
        grid=(blocks, TOKENS // tile),
        in_specs=[
            pl.BlockSpec((tile, D), lambda j, i: (i, 0)),
            pl.BlockSpec((BLOCK, D), lambda j, i: (first + j, 0)),
            pl.BlockSpec((tile, D), lambda j, i: (i, 0)),
            pl.BlockSpec((D, 2 * BLOCK), lambda j, i: (0, first + j))
            if again
            else pl.BlockSpec((tile, 2 * BLOCK), lambda j, i: (i, first + j)),
            *[pl.BlockSpec(memory_space=pl.ANY) for _ in before],
        ],
        out_specs=[
            pl.BlockSpec((tile, 2 * BLOCK), lambda j, i: (i, j)),
            pl.BlockSpec((D, 2 * BLOCK), lambda j, i: (0, j)),
            *[pl.BlockSpec((BLOCK, D), lambda j, i: (first + j, 0)) for _ in spare],
        ],
        out_shape=[
            jax.ShapeDtypeStruct((TOKENS, 2 * BLOCK * blocks), BF16),
            jax.ShapeDtypeStruct((D, 2 * BLOCK * blocks), BF16),
            *spare,
        ],
        scratch_shapes=[
            pltpu.VMEM((D, 2 * BLOCK), F32),
            *([pltpu.VMEM((tile, BLOCK), BF16), pltpu.VMEM((BLOCK, D), F32)] if with_d else []),
        ],
        compiler_params=params("arbitrary", "arbitrary"),
        cost_estimate=cost((6 if again else 4) * MM * blocks // BLOCKS, TOKENS * FF * (4 if again else 12) * blocks // BLOCKS),
        input_output_aliases={4: 2} if before else {},
        name="back",
    )(dy, wd, a, gu, *before)


def grad_down_kernel(p_ref, dy_ref, dw_ref):
    dw_ref[:, :512] = tn(p_ref[...], dy_ref[:, :512]).astype(BF16)
    dw_ref[:, 512:] = tn(dy_ref[:, 512:], p_ref[...]).T.astype(BF16)


def grad_down(p, dy):
    return pl.pallas_call(
        grad_down_kernel,
        grid=(BLOCKS,),
        in_specs=[
            pl.BlockSpec((TOKENS, BLOCK), lambda j: (0, j)),
            pl.BlockSpec((TOKENS, D), lambda j: (0, 0), pipeline_mode=pl.Buffered(1)),
        ],
        out_specs=pl.BlockSpec((BLOCK, D), lambda j: (j, 0)),
        out_shape=jax.ShapeDtypeStruct((FF, D), BF16),
        compiler_params=params("arbitrary"),
        cost_estimate=cost(MM, TOKENS * FF * 2),
        name="grad_down",
    )(p, dy)


def grad_in_kernel(split, one_ref, two_ref, w_ref, h_ref, dy_ref, dh_ref):
    da = nt(w_ref[:, :split], one_ref[...]) + nt(w_ref[:, split:], two_ref[...])
    da = da.T.astype(BF16).astype(F32)
    wide = h_ref[...].astype(F32)
    scale = scale_of(wide)
    dot = jnp.mean(da * wide, -1, keepdims=True)
    by_wide = da * scale - wide * (scale * scale * scale * dot)
    dh_ref[...] = dy_ref[...] + by_wide.astype(BF16)


def grad_in(one, two, w, h, dy, tile=512):
    row = pl.BlockSpec((tile, D), lambda i: (i, 0))
    split = one.shape[1]
    return pl.pallas_call(
        functools.partial(grad_in_kernel, split),
        grid=(TOKENS // tile,),
        in_specs=[
            pl.BlockSpec((tile, split), lambda i: (i, 0)),
            pl.BlockSpec((tile, 2 * FF - split), lambda i: (i, 0)),
            pl.BlockSpec((D, 2 * FF), lambda i: (0, 0), pipeline_mode=pl.Buffered(1)),
            row,
            row,
        ],
        out_specs=row,
        out_shape=jax.ShapeDtypeStruct((TOKENS, D), BF16),
        compiler_params=params("arbitrary"),
        cost_estimate=cost(2 * MM, TOKENS * FF * 4),
        name="grad_in",
    )(one, two, w, h, dy)


def apart(both):
    parts = [both[:, j * BLOCK : (j + 1) * BLOCK] for j in range(2 * BLOCKS)]
    return jnp.concatenate(parts[0::2], 1), jnp.concatenate(parts[1::2], 1)


def scatter(dw):
    return lax.psum_scatter(dw, "dp", scatter_dimension=0, tiled=True)


FIRST = 3


def solution(mesh):
    def gathered(w):
        return lax.all_gather(w, "dp", axis=0, tiled=True)

    def step(x, dy, w_gate, w_up, w_down):
        h0, dy = x[0], dy[0]
        d0, d1 = gathered(w_down[0]), gathered(w_down[1])
        gu0, p0, a0, w0, w1 = gate_up(h0, w_gate, w_up)
        w0, w1 = w0.reshape(D, 2 * FF), w1.reshape(D, 2 * FF)
        h1, a1 = down(p0, d0, h0)

        one1, dw, dd = back(dy, d1, a1, w1, True, True, 0, FIRST)
        by_one1 = scatter(dw)
        two1, dw, dd = back(dy, d1, a1, w1, True, True, FIRST, BLOCKS - FIRST, dd)
        by_two1 = scatter(dw)
        by_d1 = scatter(dd)
        one1, by_one1 = lax.optimization_barrier((one1, by_one1))
        dh1 = grad_in(one1, two1, w1, h1, dy)

        dd = grad_down(p0, dh1)
        by_d0 = scatter(dd)
        dh1, dd, by_two1 = lax.optimization_barrier((dh1, dd, by_two1))
        one0, dw = back(dh1, d0, a0, gu0, False, False, 0, FIRST)
        by_one0 = scatter(dw)
        dh1, dw, by_d1 = lax.optimization_barrier((dh1, dw, by_d1))
        two0, dw = back(dh1, d0, a0, gu0, False, False, FIRST, BLOCKS - FIRST)
        by_two0 = scatter(dw)
        one0, dw, by_d0 = lax.optimization_barrier((one0, dw, by_d0))
        dx = grad_in(one0, two0, w0, h0, dh1)
        g0, u0 = apart(jnp.concatenate([by_one0, by_two0], 1))
        g1, u1 = apart(jnp.concatenate([by_one1, by_two1], 1))
        return dx[None], jnp.stack([g0, g1]), jnp.stack([u0, u1]), jnp.stack([by_d0, by_d1])

    tokens = P(("rep", "dp"), None, None)
    weights = P(None, "dp", None)
    return jax.shard_map(
        step,
        mesh=mesh,
        in_specs=(tokens, tokens, weights, weights, weights),
        out_specs=(tokens,) + (P("rep", "dp", None),) * 3,
        check_vma=False,
    )
```
